32 devices in a mesh: dp: 8 (over z, y), mp: 4 (over x, core).
Axes of the slice: x: 2, y: 2, z: 4, core: 2. Of those that a mesh axis runs over, the one named last changes fastest.
Arguments:
- gradients: bfloat16 [4, 16, 1024, 1024], P(None, 'mp', 'dp'), as said below
- statistics: float32 [4, 32, 1024, 1024], P('mp', 'dp'), as said below
- accumulator: float32 [4, 16, 1024, 1024], P(None, 'mp', 'dp'), may hold values from 0.25 to 4
Outputs:
- update: float32 [4, 16, 1024, 1024], P(None, 'mp', 'dp')
- statistics_new: float32 [4, 32, 1024, 1024], P('mp', 'dp')
- accumulator_new: float32 [4, 16, 1024, 1024], P(None, 'mp', 'dp')
The draws below stay inside these ranges and needn't reach their ends.
Inputs may be any that keep to these rules, and one draw needn't show every extreme that they name: `gradients`: Real-valued gradient blocks. `statistics`: each 1024 x 1024 statistic is symmetric positive definite.
All inputs are finite; a program needn't handle non-finite values.
Results may differ from the reference program's by a relative error of at most 0.005.
The reference program's roundings to bfloat16 on the way count: a program that leaves them out, or rounds other values in their place, can miss the bound.
Values may be sent and summed in bfloat16 or wider, within the bound.
A program may use at most 192 MiB of HBM per device.

```python
import math
import jax
import jax.numpy as jnp
from jax import lax

B = 1024
ITERS = 3
RB = 4
CB = 16
CB_MP = 4
BLKS = 16
N_MP = 4


def draw_gradients(key, part):
    subkeys = jax.random.split(key, 3)
    gaussian = jax.random.normal(subkeys[0], (RB, CB, B, B), jnp.float32)
    row_scale = 10.0 ** jax.random.uniform(subkeys[1], (RB, CB, B, 1), jnp.float32)
    col_scale = 10.0 ** jax.random.uniform(subkeys[2], (RB, CB, 1, B), jnp.float32)
    rising = (3.0 ** (jnp.arange(B, dtype=jnp.float32) / B))[:, None]
    values = gaussian * row_scale * col_scale * rising
    return values.astype(jnp.bfloat16)


def draw_statistics(key, part):
    spread = 2.0

    def one_matrix(position):
        matrix_key = jax.random.fold_in(key, position)
        noise_key, scale_key = jax.random.split(matrix_key)
        gaussian = jax.random.normal(noise_key, (B, B), jnp.float32)
        wishart = jnp.dot(gaussian, gaussian.T, precision=lax.Precision.HIGHEST) / B + 0.5 * jnp.eye(B, dtype=jnp.float32)
        diagonal_scale = jnp.exp(jax.random.uniform(scale_key, (B,), jnp.float32) * jnp.log(spread))
        return 0.25 * diagonal_scale[:, None] * wishart * diagonal_scale[None, :]
    matrices = lax.map(one_matrix, jnp.arange(N_MP * 2 * BLKS, dtype=jnp.int32))
    return matrices.reshape(N_MP, 2 * BLKS, B, B)


def shard_levels(own_key, extent, cuts, smallest, high):
    def one(dim, blocks):
        heights = jax.random.uniform(jax.random.fold_in(jax.random.fold_in(own_key, 6), dim), (blocks,), jnp.float32, smallest / len(cuts), high / len(cuts))
        return jnp.repeat(jnp.exp(heights), extent[dim] // blocks).reshape((-1,) + (1,) * (len(extent) - dim - 1))

    factor_of = one(*cuts[0])
    for cut in cuts[1:]:
        factor_of = factor_of * one(*cut)
    return factor_of


def setup_inputs(seed: int = 0) -> dict:
    streams_of = jax.random.split(jax.random.key(seed), 4)
    gradients = draw_gradients(jax.random.fold_in(streams_of[3], 71), 0)
    statistics = draw_statistics(jax.random.fold_in(streams_of[3], 71), 0)
    accumulator = jnp.clip(jnp.exp(math.log(4.0) - 2.7725887 * jax.random.uniform(streams_of[2], (RB, CB, B, B), jnp.float32) ** shard_levels(streams_of[2], (RB, CB, B, B), ((1, 4), (2, 8)), -0.2, 0.2)), 0.25, 4.0)
    return {"gradients": gradients, "statistics": statistics, "accumulator": accumulator}


def matmul(left, right):
    return jnp.dot(left.astype(jnp.float32), right.astype(jnp.float32), precision=lax.Precision.HIGHEST)

def inverse_root(statistic):
    identity = jnp.eye(statistic.shape[0], dtype=jnp.float32)
    frob_norm = jnp.sqrt(jnp.sum(statistic * statistic) + 1e-06)
    newton_scale = 2.5 / frob_norm
    matrix = newton_scale * statistic
    root_iter = jnp.sqrt(jnp.sqrt(newton_scale)) * identity
    for iteration in range(ITERS):
        factor = (1.25 * identity - 0.25 * matrix).astype(jnp.bfloat16)
        root_iter = matmul(root_iter.astype(jnp.bfloat16), factor)
        if iteration + 1 < ITERS:
            square = matmul(factor, factor).astype(jnp.bfloat16)
            fourth = matmul(square, square).astype(jnp.bfloat16)
            matrix = matmul(fourth, matrix.astype(jnp.bfloat16))
    return root_iter

def reference(gradients, statistics, accumulator):
    grads_wide = gradients.astype(jnp.float32)
    grad_total = jnp.sum(grads_wide * grads_wide)
    clip_factor = jnp.minimum(1.0, jnp.sqrt(RB * CB * B * B / (grad_total + 1e-06)))

    def one_block(position):
        mp_shard = position // BLKS
        local_block = position % BLKS
        row_block = (local_block // CB_MP).astype(jnp.int32)
        col_block = (mp_shard * CB_MP + local_block % CB_MP).astype(jnp.int32)
        zero_index = jnp.zeros((), jnp.int32)
        grad_block = lax.dynamic_slice(gradients, (row_block, col_block, zero_index, zero_index), (1, 1, B, B))[0, 0]
        stat_pair = lax.dynamic_slice(statistics, (mp_shard.astype(jnp.int32), (2 * local_block).astype(jnp.int32), zero_index, zero_index), (1, 2, B, B))[0]
        left_stat = 0.9 * stat_pair[0] + 0.1 / B * clip_factor * clip_factor * matmul(grad_block, grad_block.T)
        right_stat = 0.9 * stat_pair[1] + 0.1 / B * clip_factor * clip_factor * matmul(grad_block.T, grad_block)
        left_root = inverse_root(left_stat).astype(jnp.bfloat16)
        right_root = inverse_root(right_stat).astype(jnp.bfloat16)
        left_applied = matmul(left_root, grad_block).astype(jnp.bfloat16)
        product = matmul(left_applied, right_root)
        return (jnp.stack([left_stat, right_stat]), product)
    stats_all, products = lax.map(one_block, jnp.arange(N_MP * BLKS, dtype=jnp.int32))
    statistics_new = stats_all.reshape(N_MP, 2 * BLKS, B, B)
    preconditioned = products.reshape(N_MP, RB, CB_MP, B, B).transpose(1, 0, 2, 3, 4).reshape(RB, CB, B, B)
    scaled = clip_factor * grads_wide
    accumulated = accumulator + scaled * scaled
    graft_step = scaled / jnp.sqrt(accumulated)
    graft_ratio = jnp.sqrt(jnp.sum(graft_step * graft_step) / (jnp.sum(preconditioned * preconditioned) + 1e-06))
    return (graft_ratio * preconditioned, statistics_new, accumulated)
```

```python
import jax
import jax.numpy as jnp
from jax import lax
from jax.experimental import pallas as pl
from jax.experimental.pallas import tpu as pltpu
from jax.sharding import PartitionSpec as P

ITERS = 3


def partner_2(value, axis, distance):
    return lax.ppermute(value, axis, [(i, i ^ 1 << distance) for i in range(lax.axis_size(axis))])


def batch_dot(left, right):
    return jnp.einsum("kij,kjl->kil", left, right, preferred_element_type=jnp.float32)


def inverse_roots(statistic):
    block_width = statistic.shape[-1]
    identity = jnp.eye(block_width, dtype=jnp.float32)
    frob_norms = jnp.sqrt(jnp.sum(statistic * statistic, axis=(1, 2)) + 1e-06)
    newton_scale = (2.5 / frob_norms)[:, None, None]
    matrix = newton_scale * statistic
    root_iter = jnp.sqrt(jnp.sqrt(newton_scale)) * identity
    for iteration in range(ITERS):
        factor = (1.25 * identity - 0.25 * matrix).astype(jnp.bfloat16)
        root_iter = batch_dot(root_iter.astype(jnp.bfloat16), factor)
        if iteration + 1 < ITERS:
            square = batch_dot(factor, factor).astype(jnp.bfloat16)
            fourth = batch_dot(square, square).astype(jnp.bfloat16)
            matrix = batch_dot(fourth, matrix.astype(jnp.bfloat16))
    return root_iter


def split_device(gradients, statistics, accumulator):
    owners = lax.axis_size("dp")
    own_index = lax.axis_index("dp")
    row_blocks, col_blocks, dev_rows, block_width = gradients.shape
    blocks = row_blocks * col_blocks
    owned_factors = statistics.shape[1]
    split_pairs = owned_factors == 1
    half_rows = dev_rows // 2
    parity = own_index % 2
    left_side = parity == 0
    by_block = gradients.reshape(blocks, dev_rows, block_width)
    grads_wide = gradients.astype(jnp.float32)
    grad_total = lax.psum(jnp.sum(grads_wide * grads_wide), ("dp", "mp"))
    entries = blocks * dev_rows * block_width * owners * lax.axis_size("mp")
    clip_factor = jnp.minimum(1.0, jnp.sqrt(entries / (grad_total + 1e-06)))
    scaled = clip_factor * grads_wide
    accumulated = accumulator + scaled * scaled
    graft_step = scaled / jnp.sqrt(accumulated)
    graft_squares = jnp.sum(graft_step * graft_step)
    row_parts = 2 if split_pairs else 1
    row_units = by_block.reshape(blocks * row_parts, dev_rows // row_parts, block_width)
    received = lax.all_to_all(row_units, "dp", split_axis=0, concat_axis=1, tiled=True)
    if split_pairs:
        partner_part = partner_2(received, "dp", 0)
        own_part = received.reshape(owners, 1, half_rows, block_width)
        partner_part = partner_part.reshape(owners, 1, half_rows, block_width)
        ordered = jnp.where(
            left_side,
            jnp.concatenate([own_part, partner_part], 1),
            jnp.concatenate([partner_part, own_part], 1),
        )
        whole_blocks = ordered.reshape(1, owners * dev_rows, block_width)
    else:
        whole_blocks = received
    transposed = jnp.swapaxes(whole_blocks, 1, 2)
    if split_pairs:
        factor_inputs = jnp.where(left_side, whole_blocks, transposed)
    else:
        factor_inputs = jnp.stack([whole_blocks, transposed], 1).reshape(
            owned_factors, block_width, block_width
        )
    gram_matrix = jnp.einsum(
        "kij,klj->kil", factor_inputs, factor_inputs, preferred_element_type=jnp.float32
    )
    statistics_new = (
        0.9 * statistics[0] + 0.1 / block_width * clip_factor * clip_factor * gram_matrix
    )
    root_values = inverse_roots(statistics_new).astype(jnp.bfloat16)
    if split_pairs:
        partner = partner_2(root_values, "dp", 0)
        left_root = jnp.where(left_side, root_values, partner)[0]
        right_root = jnp.where(left_side, partner, root_values)[0]
        left_rows = lax.dynamic_slice_in_dim(
            left_root.reshape(owners, 2, half_rows, block_width), parity, 1, 1
        )
        left_rows = left_rows.reshape(owners * half_rows, block_width)
        left_applied = jnp.dot(
            left_rows, whole_blocks[0], preferred_element_type=jnp.float32
        ).astype(jnp.bfloat16)
        product = jnp.dot(left_applied, right_root, preferred_element_type=jnp.float32)
        pieces = product.reshape(1, owners, half_rows, block_width)
    else:
        root_pairs = root_values.reshape(-1, 2, block_width, block_width)
        left_applied = batch_dot(root_pairs[:, 0], whole_blocks).astype(jnp.bfloat16)
        product = batch_dot(left_applied, root_pairs[:, 1])
        pieces = product.reshape(-1, owners, dev_rows, block_width)
    returned = lax.all_to_all(
        pieces.astype(jnp.bfloat16), "dp", split_axis=1, concat_axis=0, tiled=True
    ).astype(pieces.dtype)
    returned = returned.reshape(row_blocks, col_blocks, dev_rows, block_width)
    graft_total, update_total = lax.psum(
        (graft_squares, jnp.sum(returned * returned)), ("dp", "mp")
    )
    graft_ratio = jnp.sqrt(graft_total / (update_total + 1e-06))
    return (graft_ratio * returned, statistics_new[None], accumulated)


TILE = 512
SYM_TILE = 256
CHUNK = 128
MESH = pl.DeviceIdType.MESH


def peer_of(index, distance):
    bit, other = 1, index
    while bit <= distance:
        if distance & bit:
            other = other + bit * (1 - 2 * ((index // bit) % 2))
        bit *= 2
    return other


def fold(squares):
    rows, width = squares.shape
    return jnp.sum(squares.reshape(rows // 8, 8, width), axis=0)


def lane_fold(sums):
    total = sums[:, :128]
    for start in range(128, sums.shape[1], 128):
        total = total + sums[:, start : start + 128]
    return total


def whole_sum(tile):
    return jnp.sum(jnp.sum(tile, axis=0, keepdims=True), axis=1, keepdims=True)


def refresh_kernel(owners, shards, dev_rows, entries, *refs):
    grad_hbm, stats_hbm, accum_hbm = refs[:3]
    out_stats, returned = refs[3:5]
    pieces = refs[5 : 5 + owners]
    ratio_ref, clip_ref = refs[5 + owners : 7 + owners]
    (stat, blocks, factor, square, fourth, mats, root, product, accum, frob, sums) = refs[
        7 + owners : 18 + owners
    ]
    (dp_clip, mp_clip, dp_ratio, mp_ratio) = refs[18 + owners : 22 + owners]
    (
        in_send, in_recv, out_send, out_recv, dp_send, dp_recv, mp_send, mp_recv,
        stage_sem, own_sem, load_sem, store_sem, piece_sem,
    ) = refs[22 + owners :]
    width = grad_hbm.shape[1]
    slots = grad_hbm.shape[0] // width
    me, shard = lax.axis_index("dp"), lax.axis_index("mp")
    dot = lambda a, b: jnp.dot(a, b, preferred_element_type=jnp.float32)
    near_first = list(range(1, owners))
    flipped = slots

    def start_all(copy_of):
        for k in near_first:
            copy_of(k).start()

    def rows_of(owner):
        return pl.ds(pl.multiple_of(owner * dev_rows, dev_rows), dev_rows)

    def unit(owner, slot):
        start = (owner * slots + slot) * dev_rows
        return grad_hbm.at[pl.ds(pl.multiple_of(start, dev_rows), dev_rows)]

    def own_rows(slot):
        return pltpu.make_async_copy(
            unit(me, slot), blocks.at[slot, rows_of(me)], own_sem.at[slot]
        )

    def rows_in(slot, k):
        return pltpu.make_async_remote_copy(
            src_ref=unit(peer_of(me, k), slot),
            dst_ref=blocks.at[slot, rows_of(me)],
            send_sem=in_send.at[slot, k],
            recv_sem=in_recv.at[slot, k],
            device_id=(peer_of(me, k), shard),
            device_id_type=MESH,
        )

    def rows_out(k):
        return pltpu.make_async_remote_copy(
            src_ref=product.at[0, rows_of(peer_of(me, k))],
            dst_ref=returned.at[rows_of(me)],
            send_sem=out_send.at[k],
            recv_sem=out_recv.at[k],
            device_id=(peer_of(me, k), shard),
            device_id_type=MESH,
        )

    def piece(k):
        source = product.at[slots - 1, rows_of(peer_of(me, k))]
        return pltpu.make_async_copy(source, pieces[k], piece_sem.at[k])

    own_out = pltpu.make_async_copy(
        product.at[0, rows_of(me)], returned.at[rows_of(me)], own_sem.at[slots]
    )

    def load(slot, s):
        return pltpu.make_async_copy(
            stats_hbm.at[2 * slot + s], stat.at[s], load_sem.at[s]
        )

    def store(slot, s):
        return pltpu.make_async_copy(
            stat.at[s], out_stats.at[2 * slot + s], store_sem.at[s]
        )

    def dp_copy(which, buffer, k):
        return pltpu.make_async_remote_copy(
            src_ref=buffer.at[me],
            dst_ref=buffer.at[me],
            send_sem=dp_send.at[which, k],
            recv_sem=dp_recv.at[which, k],
            device_id=(peer_of(me, k), shard),
            device_id_type=MESH,
        )

    def mp_copy(which, buffer, k):
        return pltpu.make_async_remote_copy(
            src_ref=buffer.at[shard],
            dst_ref=buffer.at[shard],
            send_sem=mp_send.at[which, k],
            recv_sem=mp_recv.at[which, k],
            device_id=(me, peer_of(shard, k)),
            device_id_type=MESH,
        )

    def send_sums(which, dp_buffer, tile):
        dp_buffer[me] = tile
        for k in near_first:
            dp_copy(which, dp_buffer, k).start()

    def total_sums(which, dp_buffer, mp_buffer):
        for k in near_first:
            dp_copy(which, dp_buffer, k).wait()
        mp_buffer[shard] = jnp.sum(dp_buffer[...], axis=0)
        for k in range(1, shards):
            mp_copy(which, mp_buffer, k).start()
        for k in range(1, shards):
            mp_copy(which, mp_buffer, k).wait()
        return jnp.sum(mp_buffer[...], axis=0)

    stage_grads = pltpu.make_async_copy(grad_hbm, factor, stage_sem.at[0])
    stage_accum = pltpu.make_async_copy(accum_hbm, accum, stage_sem.at[1])
    stage_grads.start()
    barrier = pltpu.get_barrier_semaphore()
    for k in range(1, owners):
        pl.semaphore_signal(
            barrier, inc=1, device_id=(peer_of(me, k), shard), device_id_type=MESH
        )
    for k in range(1, shards):
        pl.semaphore_signal(
            barrier, inc=1, device_id=(me, peer_of(shard, k)), device_id_type=MESH
        )
    pl.semaphore_wait(barrier, owners + shards - 2)

    stage_grads.wait()
    sums[0] = jnp.zeros((8, width), jnp.float32)

    @pl.loop(0, slots * width // CHUNK)
    def _(i):
        rows = pl.ds(pl.multiple_of(i * CHUNK, CHUNK), CHUNK)
        wide = factor[rows, :].astype(jnp.float32)
        sums[0] += fold(wide * wide)

    send_sums(0, dp_clip, lane_fold(sums[0]))
    start_all(lambda k: rows_in(0, k))
    for slot in range(slots):
        own_rows(slot).start()
    stage_accum.start()
    for s in range(2):
        load(0, s).start()

    grad_total = whole_sum(total_sums(0, dp_clip, mp_clip))
    clip_factor = jnp.minimum(1.0, jnp.sqrt(entries / (grad_total + 1e-06)))
    clip_ref[...] = jnp.broadcast_to(clip_factor, clip_ref.shape)
    sums[0] = jnp.zeros((8, width), jnp.float32)
    sums[1] = jnp.zeros((8, width), jnp.float32)
    stage_accum.wait()

    @pl.loop(0, slots * width // CHUNK)
    def _(i):
        rows = pl.ds(pl.multiple_of(i * CHUNK, CHUNK), CHUNK)
        scaled = clip_ref[0:1, 0:1] * factor[rows, :].astype(jnp.float32)
        graft_step = scaled / jnp.sqrt(accum[rows, :] + scaled * scaled)
        sums[1] += fold(graft_step * graft_step)

    def panels(tile):
        return [(start, start + tile) for start in range(0, width, tile)]

    def diagonal(rows, cols):
        row_ids = lax.broadcasted_iota(jnp.int32, (rows, cols), 0)
        return row_ids == lax.broadcasted_iota(jnp.int32, (rows, cols), 1)

    def mirrored(write, left, right):
        for start, stop in panels(min(SYM_TILE, width)):
            upper = dot(left[start:stop, :], right[:, start:])
            write(start, stop, upper)

    def keep(target, start, stop, value):
        target[start:stop, start:] = value
        if stop < width:
            target[stop:, start:stop] = value[:, stop - start :].T

    @pl.loop(0, slots)
    def _(slot):
        own_rows(slot).wait()
        for k in range(owners):
            if k:
                rows_in(slot, k).wait_recv()
            rows = rows_of(peer_of(me, k))
            blocks[flipped, :, rows] = blocks[slot, rows, :].T

        @pl.when(slot + 1 < slots)
        def _():
            start_all(lambda k: rows_in(slot + 1, k))

        @pl.when(slot == 1)
        def _():
            start_all(rows_out)
            own_out.start()

        for s in range(2):
            load(slot, s).wait()

        @pl.loop(0, 2)
        def _(s):
            left = blocks.at[slot + s * (flipped - slot)]
            right = blocks.at[flipped - s * (flipped - slot)]
            old = stat.at[s]
            clip = clip_ref[0:1, 0:1]
            scale = 0.1 / width * clip * clip
            frob[s] = jnp.zeros((8, width), jnp.float32)

            def write(start, stop, upper):
                part = scale * upper
                new = 0.9 * old[start:stop, start:] + part
                old[start:stop, start:] = new
                frob[s, :, start:] += fold(new * new)
                if stop < width:
                    new = 0.9 * old[stop:, start:stop] + part[:, stop - start :].T
                    old[stop:, start:stop] = new
                    frob[s, :, start:stop] += fold(new * new)

            mirrored(write, left, right)
            store(slot, s).start()

        @pl.loop(0, 2)
        def _(s):
            newton_scale = 2.5 / jnp.sqrt(whole_sum(frob[s]) + 1e-06)
            first_root = jnp.sqrt(jnp.sqrt(newton_scale))
            first_root = first_root.astype(jnp.bfloat16).astype(jnp.float32)

            @pl.loop(0, width // CHUNK)
            def _(i):
                row = pl.multiple_of(i * CHUNK, CHUNK)
                rows = pl.ds(row, CHUNK)
                wide = pl.ds(pl.multiple_of(s * width + row, CHUNK), CHUNK)
                row_ids = lax.broadcasted_iota(jnp.int32, (CHUNK, width), 0) + row
                on_diagonal = row_ids == lax.broadcasted_iota(jnp.int32, (CHUNK, width), 1)
                matrix = newton_scale * stat[s, rows, :]
                quarter = -0.25 * matrix
                value = jnp.where(on_diagonal, 1.25 + quarter, quarter).astype(jnp.bfloat16)
                factor[wide, :] = value
                root[0, s, rows, :] = (first_root * value.astype(jnp.float32)).astype(
                    jnp.bfloat16
                )
                mats[0, s, rows, :] = matrix.astype(jnp.bfloat16)

        @pl.loop(0, ITERS - 1)
        def _(step):
            now = lax.rem(step, 2)
            later = 1 - now

            def each(body):
                @pl.loop(0, 2)
                def _(s):
                    body(s, factor.at[pl.ds(pl.multiple_of(s * width, width), width)])

            def squared(s, own):
                def write(start, stop, upper):
                    keep(square.at[s], start, stop, upper.astype(jnp.bfloat16))

                mirrored(write, own, own)

            def power(s, own):
                def write(start, stop, upper):
                    keep(fourth.at[s], start, stop, upper.astype(jnp.bfloat16))

                mirrored(write, square.at[s], square.at[s])

            def next_matrix(s, own):
                def write(start, stop, upper):
                    quarter = -0.25 * upper
                    on_diagonal = diagonal(*upper.shape)
                    value = jnp.where(on_diagonal, 1.25 + quarter, quarter)
                    keep(own, start, stop, value.astype(jnp.bfloat16))
                    keep(mats.at[later, s], start, stop, upper.astype(jnp.bfloat16))

                mirrored(write, fourth.at[s], mats.at[now, s])

            def next_root(s, own):
                def write(start, stop, upper):
                    keep(root.at[later, s], start, stop, upper.astype(jnp.bfloat16))

                mirrored(write, root.at[now, s], own)

            each(squared)
            each(power)
            each(next_matrix)
            each(next_root)

        for s in range(2):
            store(slot, s).wait()

        @pl.when(slot + 1 < slots)
        def _():
            for s in range(2):
                load(slot + 1, s).start()

        last = (ITERS - 1) % 2
        for start, stop in panels(min(TILE, width)):
            applied = dot(root[last, 0, start:stop, :], blocks[slot])
            blocks[flipped, start:stop, :] = applied.astype(jnp.bfloat16)
        for start, stop in panels(min(TILE, width)):
            value = dot(blocks[flipped, start:stop, :], root[last, 1])
            product[slot, start:stop, :] = value.astype(jnp.bfloat16)
            sums[0] += fold(value * value)

        @pl.when(slot == slots - 1)
        def _():
            for k in range(owners):
                piece(k).start()

    both = jnp.concatenate([lane_fold(sums[0]), lane_fold(sums[1])], axis=0)
    send_sums(1, dp_ratio, both)
    totals = total_sums(1, dp_ratio, mp_ratio)
    ratio = jnp.sqrt(whole_sum(totals[8:]) / (whole_sum(totals[:8]) + 1e-06))
    ratio_ref[...] = jnp.broadcast_to(ratio, ratio_ref.shape)
    for k in near_first:
        for slot in range(slots):
            rows_in(slot, k).wait_send()
        rows_out(k).wait()
    own_out.wait()
    for k in range(owners):
        piece(k).wait()


def refresh(gradients, statistics, accumulator, owners, shards, entries):
    slots = statistics.shape[0] // 2
    dev_rows, width = gradients.shape[-2:]
    hbm = pl.BlockSpec(memory_space=pl.ANY)
    vmem = pl.BlockSpec(memory_space=pltpu.VMEM)
    tile = jax.ShapeDtypeStruct((8, 128), jnp.float32)
    dma = pltpu.SemaphoreType.DMA
    bf16 = lambda *lead: pltpu.VMEM((*lead, width, width), jnp.bfloat16)
    f32 = lambda *shape: pltpu.VMEM(shape, jnp.float32)
    return pl.pallas_call(
        lambda *refs: refresh_kernel(owners, shards, dev_rows, entries, *refs),
        out_shape=(
            jax.ShapeDtypeStruct(statistics.shape, jnp.float32),
            jax.ShapeDtypeStruct((width, width), jnp.bfloat16),
            *[jax.ShapeDtypeStruct((dev_rows, width), jnp.bfloat16)] * owners,
            tile,
            tile,
        ),
        in_specs=[hbm] * 3,
        out_specs=(hbm, hbm, *[hbm] * owners, vmem, vmem),
        scratch_shapes=[
            f32(2, width, width),
            bf16(slots + 1),
            pltpu.VMEM((2 * width, width), jnp.bfloat16),
            bf16(2),
            bf16(2),
            bf16(2, 2),
            bf16(2, 2),
            bf16(slots),
            f32(slots * width, width),
            f32(2, 8, width),
            f32(2, 8, width),
            f32(owners, 8, 128),
            f32(shards, 8, 128),
            f32(owners, 16, 128),
            f32(shards, 16, 128),
            dma((slots, owners)),
            dma((slots, owners)),
            dma((owners,)),
            dma((owners,)),
            dma((2, owners)),
            dma((2, owners)),
            dma((2, shards)),
            dma((2, shards)),
            dma((2,)),
            dma((slots + 1,)),
            dma((2,)),
            dma((2,)),
            dma((owners,)),
        ],
        compiler_params=pltpu.CompilerParams(
            collective_id=0, has_side_effects=True, vmem_limit_bytes=63 * 2**20
        ),
        cost_estimate=pl.CostEstimate(
            flops=60 * width**3, bytes_accessed=40 * width**2, transcendentals=0
        ),
        name="refresh",
    )(
        gradients.reshape(slots * width, width),
        statistics,
        accumulator.reshape(slots * width, width),
    )


def settle_kernel(ratio_ref, clip_ref, stats_ref, grad_ref, accum_ref, back_ref, *outs):
    stats_out, accum_out, update_out = outs
    stats_out[...] = stats_ref[...]
    scaled = clip_ref[0:1, 0:1] * grad_ref[...].astype(jnp.float32)
    accum_out[...] = accum_ref[...] + scaled * scaled
    update_out[0, 0] = ratio_ref[0:1, 0:1] * back_ref[...].astype(jnp.float32)


def settle(ratio, clip, stats, grads, accum, returned, owners, slots):
    factors, width, _ = stats.shape
    dev_rows = width // owners
    steps = 2 * owners
    stat_rows = factors * width // steps
    per_stat = width // stat_rows
    half = dev_rows // 2
    rows = lambda count: pl.BlockSpec((count, width), lambda i: (i, 0))
    tile = pl.BlockSpec((8, 128), lambda i: (0, 0))
    stat = pl.BlockSpec((1, stat_rows, width), lambda i: (i // per_stat, i % per_stat, 0))
    grad_rows = grads.shape[0] // steps
    return pl.pallas_call(
        settle_kernel,
        grid=(steps,),
        out_shape=(
            jax.ShapeDtypeStruct(stats.shape, jnp.float32),
            jax.ShapeDtypeStruct(accum.shape, jnp.float32),
            jax.ShapeDtypeStruct((owners, slots, dev_rows, width), jnp.float32),
        ),
        in_specs=[tile, tile, stat, rows(grad_rows), rows(grad_rows), rows(half)],
        out_specs=(
            stat,
            rows(grad_rows),
            pl.BlockSpec((1, 1, half, width), lambda i: (i // 2, 0, i % 2, 0)),
        ),
        cost_estimate=pl.CostEstimate(
            flops=40 * width**3 // 4, bytes_accessed=58 * width**2, transcendentals=0
        ),
        name="settle",
    )(ratio, clip, stats, grads, accum, returned)


def scale_rest_kernel(distances, slot, ratio_ref, *refs):
    count = len(distances)
    arrived = refs[:count]
    out = refs[count + 1]
    wide, out_sem = refs[count + 2 :]
    me = lax.axis_index("dp")
    stores = []
    for i, k in enumerate(distances):
        wide[i] = ratio_ref[0:1, 0:1] * arrived[i][...].astype(jnp.float32)
        stores.append(
            pltpu.make_async_copy(wide.at[i], out.at[peer_of(me, k), slot], out_sem.at[i])
        )
        stores[-1].start()
    for copy in stores:
        copy.wait()


def scale_rest(ratio, arrived, distances, slot, update):
    count = len(arrived)
    dev_rows, width = arrived[0].shape
    hbm = pl.BlockSpec(memory_space=pl.ANY)
    vmem = pl.BlockSpec(memory_space=pltpu.VMEM)
    return pl.pallas_call(
        lambda *refs: scale_rest_kernel(distances, slot, *refs),
        out_shape=jax.ShapeDtypeStruct(update.shape, jnp.float32),
        in_specs=[vmem] * (count + 1) + [hbm],
        out_specs=hbm,
        scratch_shapes=[
            pltpu.VMEM((count, dev_rows, width), jnp.float32),
            pltpu.SemaphoreType.DMA((count,)),
        ],
        input_output_aliases={count + 1: 0},
        cost_estimate=pl.CostEstimate(
            flops=count * dev_rows * width,
            bytes_accessed=6 * count * dev_rows * width,
            transcendentals=0,
        ),
        name="scale_rest",
    )(ratio, *arrived, update)


def power_of_two(count):
    return count >= 2 and count & (count - 1) == 0


def on_device(gradients, statistics, accumulator):
    owned_factors = statistics.shape[1]
    owners, shards = lax.axis_size("dp"), lax.axis_size("mp")
    row_blocks, col_blocks, dev_rows, block_width = gradients.shape
    paired = owned_factors == 4 and power_of_two(owners) and power_of_two(shards)
    if not paired or dev_rows % CHUNK or block_width % TILE:
        return split_device(gradients, statistics, accumulator)
    slots = owned_factors // 2
    blocks = row_blocks * col_blocks
    entries = float(blocks * dev_rows * block_width * owners * shards)
    results = refresh(gradients, statistics[0], accumulator, owners, shards, entries)
    statistics_new, returned = results[:2]
    pieces = results[2 : 2 + owners]
    ratio, clip = results[2 + owners :]
    arrived = {0: pieces[0]}
    for k in range(1, owners):
        pairs = [(i, i ^ k) for i in range(owners)]
        arrived[k] = lax.ppermute(pieces[k], "dp", pairs)
    flat = lambda value: value.reshape(slots * block_width, block_width)
    statistics_new, accumulated, update = settle(
        ratio, clip, statistics_new, flat(gradients), flat(accumulator), returned, owners, slots
    )
    near = list(range(owners // 2))
    far = list(range(owners // 2, owners))
    for group in (near, far):
        update = scale_rest(ratio, [arrived[k] for k in group], group, slots - 1, update)
    update = update.reshape(gradients.shape)
    return (update, statistics_new[None], accumulated.reshape(accumulator.shape))


def solution(mesh):
    return jax.shard_map(
        on_device,
        mesh=mesh,
        in_specs=(P(None, "mp", "dp", None), P("mp", "dp", None, None), P(None, "mp", "dp", None)),
        out_specs=(P(None, "mp", "dp", None), P("mp", "dp", None, None), P(None, "mp", "dp", None)),
        check_vma=False,
    )
```

```python
import jax
import jax.numpy as jnp
from jax import lax
from jax.experimental import pallas as pl
from jax.experimental.pallas import tpu as pltpu
from jax.sharding import PartitionSpec as P

ITERS = 3


def partner_2(value, axis, distance):
    return lax.ppermute(value, axis, [(i, i ^ 1 << distance) for i in range(lax.axis_size(axis))])


def batch_dot(left, right):
    return jnp.einsum("kij,kjl->kil", left, right, preferred_element_type=jnp.float32)


def inverse_roots(statistic):
    block_width = statistic.shape[-1]
    identity = jnp.eye(block_width, dtype=jnp.float32)
    frob_norms = jnp.sqrt(jnp.sum(statistic * statistic, axis=(1, 2)) + 1e-06)
    newton_scale = (2.5 / frob_norms)[:, None, None]
    matrix = newton_scale * statistic
    root_iter = jnp.sqrt(jnp.sqrt(newton_scale)) * identity
    for iteration in range(ITERS):
        factor = (1.25 * identity - 0.25 * matrix).astype(jnp.bfloat16)
        root_iter = batch_dot(root_iter.astype(jnp.bfloat16), factor)
        if iteration + 1 < ITERS:
            square = batch_dot(factor, factor).astype(jnp.bfloat16)
            fourth = batch_dot(square, square).astype(jnp.bfloat16)
            matrix = batch_dot(fourth, matrix.astype(jnp.bfloat16))
    return root_iter


def split_device(gradients, statistics, accumulator):
    owners = lax.axis_size("dp")
    own_index = lax.axis_index("dp")
    row_blocks, col_blocks, dev_rows, block_width = gradients.shape
    blocks = row_blocks * col_blocks
    owned_factors = statistics.shape[1]
    split_pairs = owned_factors == 1
    half_rows = dev_rows // 2
    parity = own_index % 2
    left_side = parity == 0
    by_block = gradients.reshape(blocks, dev_rows, block_width)
    grads_wide = gradients.astype(jnp.float32)
    grad_total = lax.psum(jnp.sum(grads_wide * grads_wide), ("dp", "mp"))
    entries = blocks * dev_rows * block_width * owners * lax.axis_size("mp")
    clip_factor = jnp.minimum(1.0, jnp.sqrt(entries / (grad_total + 1e-06)))
    scaled = clip_factor * grads_wide
    accumulated = accumulator + scaled * scaled
    graft_step = scaled / jnp.sqrt(accumulated)
    graft_squares = jnp.sum(graft_step * graft_step)
    row_parts = 2 if split_pairs else 1
    row_units = by_block.reshape(blocks * row_parts, dev_rows // row_parts, block_width)
    received = lax.all_to_all(row_units, "dp", split_axis=0, concat_axis=1, tiled=True)
    if split_pairs:
        partner_part = partner_2(received, "dp", 0)
        own_part = received.reshape(owners, 1, half_rows, block_width)
        partner_part = partner_part.reshape(owners, 1, half_rows, block_width)
        ordered = jnp.where(
            left_side,
            jnp.concatenate([own_part, partner_part], 1),
            jnp.concatenate([partner_part, own_part], 1),
        )
        whole_blocks = ordered.reshape(1, owners * dev_rows, block_width)
    else:
        whole_blocks = received
    transposed = jnp.swapaxes(whole_blocks, 1, 2)
    if split_pairs:
        factor_inputs = jnp.where(left_side, whole_blocks, transposed)
    else:
        factor_inputs = jnp.stack([whole_blocks, transposed], 1).reshape(
            owned_factors, block_width, block_width
        )
    gram_matrix = jnp.einsum(
        "kij,klj->kil", factor_inputs, factor_inputs, preferred_element_type=jnp.float32
    )
    statistics_new = (
        0.9 * statistics[0] + 0.1 / block_width * clip_factor * clip_factor * gram_matrix
    )
    root_values = inverse_roots(statistics_new).astype(jnp.bfloat16)
    if split_pairs:
        partner = partner_2(root_values, "dp", 0)
        left_root = jnp.where(left_side, root_values, partner)[0]
        right_root = jnp.where(left_side, partner, root_values)[0]
        left_rows = lax.dynamic_slice_in_dim(
            left_root.reshape(owners, 2, half_rows, block_width), parity, 1, 1
        )
        left_rows = left_rows.reshape(owners * half_rows, block_width)
        left_applied = jnp.dot(
            left_rows, whole_blocks[0], preferred_element_type=jnp.float32
        ).astype(jnp.bfloat16)
        product = jnp.dot(left_applied, right_root, preferred_element_type=jnp.float32)
        pieces = product.reshape(1, owners, half_rows, block_width)
    else:
        root_pairs = root_values.reshape(-1, 2, block_width, block_width)
        left_applied = batch_dot(root_pairs[:, 0], whole_blocks).astype(jnp.bfloat16)
        product = batch_dot(left_applied, root_pairs[:, 1])
        pieces = product.reshape(-1, owners, dev_rows, block_width)
    returned = lax.all_to_all(
        pieces.astype(jnp.bfloat16), "dp", split_axis=1, concat_axis=0, tiled=True
    ).astype(pieces.dtype)
    returned = returned.reshape(row_blocks, col_blocks, dev_rows, block_width)
    graft_total, update_total = lax.psum(
        (graft_squares, jnp.sum(returned * returned)), ("dp", "mp")
    )
    graft_ratio = jnp.sqrt(graft_total / (update_total + 1e-06))
    return (graft_ratio * returned, statistics_new[None], accumulated)


TILE = 512
FINE_TILE = 256
CHUNK = 128
MESH = pl.DeviceIdType.MESH


def peer_of(index, distance):
    bit, other = 1, index
    while bit <= distance:
        if distance & bit:
            other = other + bit * (1 - 2 * ((index // bit) % 2))
        bit *= 2
    return other


def fold(squares):
    rows, width = squares.shape
    return jnp.sum(squares.reshape(rows // 8, 8, width), axis=0)


def lane_fold(sums):
    total = sums[:, :128]
    for start in range(128, sums.shape[1], 128):
        total = total + sums[:, start : start + 128]
    return total


def whole_sum(tile):
    return jnp.sum(jnp.sum(tile, axis=0, keepdims=True), axis=1, keepdims=True)


def refresh_kernel(owners, shards, dev_rows, entries, *refs):
    grad_hbm, stats_hbm, accum_hbm = refs[:3]
    out_stats, returned = refs[3:5]
    pieces = refs[5 : 5 + owners]
    ratio_ref, clip_ref = refs[5 + owners : 7 + owners]
    (stat, blocks, factor, square, fourth, mats, root, product, accum, frob, sums) = refs[
        7 + owners : 18 + owners
    ]
    (dp_clip, mp_clip, dp_ratio, mp_ratio) = refs[18 + owners : 22 + owners]
    (
        in_send, in_recv, out_send, out_recv, dp_send, dp_recv, mp_send, mp_recv,
        stage_sem, own_sem, load_sem, store_sem, piece_sem, turn_sem,
    ) = refs[22 + owners :]
    width = grad_hbm.shape[1]
    slots = grad_hbm.shape[0] // width
    me, shard = lax.axis_index("dp"), lax.axis_index("mp")
    dot = lambda a, b: jnp.dot(a, b, preferred_element_type=jnp.float32)
    near_first = list(range(1, owners))
    partner = peer_of(me, max(1, owners // 4))
    flipped = slots

    def start_all(copy_of):
        for k in near_first:
            copy_of(k).start()

    def rows_of(owner):
        return pl.ds(pl.multiple_of(owner * dev_rows, dev_rows), dev_rows)

    def unit(owner, slot):
        start = (owner * slots + slot) * dev_rows
        return grad_hbm.at[pl.ds(pl.multiple_of(start, dev_rows), dev_rows)]

    def own_rows(slot):
        return pltpu.make_async_copy(
            unit(me, slot), blocks.at[slot, rows_of(me)], own_sem.at[slot]
        )

    def rows_in(slot, k):
        return pltpu.make_async_remote_copy(
            src_ref=unit(peer_of(me, k), slot),
            dst_ref=blocks.at[slot, rows_of(me)],
            send_sem=in_send.at[slot, k],
            recv_sem=in_recv.at[slot, k],
            device_id=(peer_of(me, k), shard),
            device_id_type=MESH,
        )

    def rows_out(k):
        return pltpu.make_async_remote_copy(
            src_ref=product.at[0, rows_of(peer_of(me, k))],
            dst_ref=returned.at[rows_of(me)],
            send_sem=out_send.at[k],
            recv_sem=out_recv.at[k],
            device_id=(peer_of(me, k), shard),
            device_id_type=MESH,
        )

    def piece(k):
        source = product.at[slots - 1, rows_of(peer_of(me, k))]
        return pltpu.make_async_copy(source, pieces[k], piece_sem.at[k])

    own_out = pltpu.make_async_copy(
        product.at[0, rows_of(me)], returned.at[rows_of(me)], own_sem.at[slots]
    )

    def load(slot, s):
        return pltpu.make_async_copy(
            stats_hbm.at[2 * slot + s], stat.at[s], load_sem.at[s]
        )

    def store(slot, s):
        return pltpu.make_async_copy(
            stat.at[s], out_stats.at[2 * slot + s], store_sem.at[s]
        )

    def dp_copy(which, buffer, k):
        return pltpu.make_async_remote_copy(
            src_ref=buffer.at[me],
            dst_ref=buffer.at[me],
            send_sem=dp_send.at[which, k],
            recv_sem=dp_recv.at[which, k],
            device_id=(peer_of(me, k), shard),
            device_id_type=MESH,
        )

    def mp_copy(which, buffer, k):
        return pltpu.make_async_remote_copy(
            src_ref=buffer.at[shard],
            dst_ref=buffer.at[shard],
            send_sem=mp_send.at[which, k],
            recv_sem=mp_recv.at[which, k],
            device_id=(me, peer_of(shard, k)),
            device_id_type=MESH,
        )

    over_dp = (dp_copy, me, near_first)
    over_mp = (mp_copy, shard, list(range(1, shards)))

    def send_sums(which, axis, buffer, tile):
        copy_of, place, distances = axis
        buffer[place] = tile
        for k in distances:
            copy_of(which, buffer, k).start()

    def total_sums(which, axis, buffer):
        copy_of, _, distances = axis
        for k in distances:
            copy_of(which, buffer, k).wait()
        return jnp.sum(buffer[...], axis=0)

    stage_grads = pltpu.make_async_copy(grad_hbm, factor, stage_sem.at[0])
    stage_accum = pltpu.make_async_copy(accum_hbm, accum, stage_sem.at[1])
    stage_grads.start()
    barrier = pltpu.get_barrier_semaphore()
    for k in range(1, owners):
        pl.semaphore_signal(
            barrier, inc=1, device_id=(peer_of(me, k), shard), device_id_type=MESH
        )
    for k in range(1, shards):
        pl.semaphore_signal(
            barrier, inc=1, device_id=(me, peer_of(shard, k)), device_id_type=MESH
        )
    pl.semaphore_wait(barrier, owners + shards - 2)

    stage_grads.wait()
    sums[0] = jnp.zeros((8, width), jnp.float32)

    @pl.loop(0, slots * width // CHUNK)
    def _(i):
        rows = pl.ds(pl.multiple_of(i * CHUNK, CHUNK), CHUNK)
        wide = factor[rows, :].astype(jnp.float32)
        sums[0] += fold(wide * wide)

    send_sums(0, over_dp, dp_clip, lane_fold(sums[0]))
    start_all(lambda k: rows_in(0, k))
    for slot in range(slots):
        own_rows(slot).start()
    stage_accum.start()
    for s in range(2):
        load(0, s).start()

    send_sums(0, over_mp, mp_clip, total_sums(0, over_dp, dp_clip))
    grad_total = whole_sum(total_sums(0, over_mp, mp_clip))
    clip_factor = jnp.minimum(1.0, jnp.sqrt(entries / (grad_total + 1e-06)))
    clip_ref[...] = jnp.broadcast_to(clip_factor, clip_ref.shape)
    sums[0] = jnp.zeros((8, width), jnp.float32)
    sums[1] = jnp.zeros((8, width), jnp.float32)
    stage_accum.wait()

    @pl.loop(0, slots * width // CHUNK)
    def _(i):
        rows = pl.ds(pl.multiple_of(i * CHUNK, CHUNK), CHUNK)
        scaled = clip_ref[0:1, 0:1] * factor[rows, :].astype(jnp.float32)
        graft_step = scaled / jnp.sqrt(accum[rows, :] + scaled * scaled)
        sums[1] += fold(graft_step * graft_step)

    def panels(tile):
        return [(start, start + tile) for start in range(0, width, tile)]

    def diagonal(rows, cols):
        row_ids = lax.broadcasted_iota(jnp.int32, (rows, cols), 0)
        return row_ids == lax.broadcasted_iota(jnp.int32, (rows, cols), 1)

    def mirrored(write, left, right, tile=FINE_TILE):
        for start, stop in panels(min(tile, width)):
            upper = dot(left[start:stop, :], right[:, start:])
            write(start, stop, upper)

    def keep(target, start, stop, value):
        target[start:stop, start:] = value
        if stop < width:
            target[stop:, start:stop] = value[:, stop - start :].T

    @pl.loop(0, slots)
    def _(slot):
        own_rows(slot).wait()
        for k in range(owners):
            if k:
                rows_in(slot, k).wait_recv()
            rows = rows_of(peer_of(me, k))
            blocks[flipped, :, rows] = blocks[slot, rows, :].T

        @pl.when(slot + 1 < slots)
        def _():
            pl.semaphore_signal(
                turn_sem, inc=1, device_id=(partner, shard), device_id_type=MESH
            )
            pl.semaphore_wait(turn_sem, 1)
            start_all(lambda k: rows_in(slot + 1, k))

        @pl.when(slot == 1)
        def _():
            start_all(rows_out)
            own_out.start()

        for s in range(2):
            load(slot, s).wait()

        @pl.loop(0, 2)
        def _(s):
            left = blocks.at[slot + s * (flipped - slot)]
            right = blocks.at[flipped - s * (flipped - slot)]
            old = stat.at[s]
            clip = clip_ref[0:1, 0:1]
            scale = 0.1 / width * clip * clip
            frob[s] = jnp.zeros((8, width), jnp.float32)

            def write(start, stop, upper):
                part = scale * upper
                new = 0.9 * old[start:stop, start:] + part
                old[start:stop, start:] = new
                frob[s, :, start:] += fold(new * new)
                if stop < width:
                    new = 0.9 * old[stop:, start:stop] + part[:, stop - start :].T
                    old[stop:, start:stop] = new
                    frob[s, :, start:stop] += fold(new * new)

            mirrored(write, left, right)
            store(slot, s).start()

        @pl.loop(0, 2)
        def _(s):
            newton_scale = 2.5 / jnp.sqrt(whole_sum(frob[s]) + 1e-06)
            first_root = jnp.sqrt(jnp.sqrt(newton_scale))
            first_root = first_root.astype(jnp.bfloat16).astype(jnp.float32)

            @pl.loop(0, width // CHUNK)
            def _(i):
                row = pl.multiple_of(i * CHUNK, CHUNK)
                rows = pl.ds(row, CHUNK)
                wide = pl.ds(pl.multiple_of(s * width + row, CHUNK), CHUNK)
                matrix = newton_scale * stat[s, rows, :]
                value = (-0.25 * matrix).astype(jnp.bfloat16)
                factor[wide, :] = value
                root[0, s, rows, :] = (first_root * value.astype(jnp.float32)).astype(
                    jnp.bfloat16
                )
                mats[0, s, rows, :] = matrix.astype(jnp.bfloat16)
                quarter = -0.25 * (newton_scale * stat[s, rows, rows])
                value = jnp.where(diagonal(CHUNK, CHUNK), 1.25 + quarter, quarter)
                value = value.astype(jnp.bfloat16)
                factor[wide, rows] = value
                root[0, s, rows, rows] = (first_root * value.astype(jnp.float32)).astype(
                    jnp.bfloat16
                )

        @pl.loop(0, ITERS - 1)
        def _(step):
            now = lax.rem(step, 2)
            later = 1 - now

            def each(body):
                @pl.loop(0, 2)
                def _(s):
                    body(s, factor.at[pl.ds(pl.multiple_of(s * width, width), width)])

            def squared(s, own):
                def write(start, stop, upper):
                    keep(square.at[s], start, stop, upper.astype(jnp.bfloat16))

                mirrored(write, own, own)

            def power(s, own):
                def write(start, stop, upper):
                    keep(fourth.at[s], start, stop, upper.astype(jnp.bfloat16))

                mirrored(write, square.at[s], square.at[s])

            def next_matrix(s, own):
                def write(start, stop, upper):
                    quarter = -0.25 * upper
                    on_diagonal = diagonal(*upper.shape)
                    value = jnp.where(on_diagonal, 1.25 + quarter, quarter)
                    keep(own, start, stop, value.astype(jnp.bfloat16))
                    keep(mats.at[later, s], start, stop, upper.astype(jnp.bfloat16))

                mirrored(write, fourth.at[s], mats.at[now, s], TILE)

            def next_root(s, own):
                def write(start, stop, upper):
                    keep(root.at[later, s], start, stop, upper.astype(jnp.bfloat16))

                mirrored(write, root.at[now, s], own, TILE)

            each(squared)
            each(power)
            each(next_matrix)
            each(next_root)

        for s in range(2):
            store(slot, s).wait()

        @pl.when(slot + 1 < slots)
        def _():
            for s in range(2):
                load(slot + 1, s).start()

        last = (ITERS - 1) % 2
        for start, stop in panels(min(TILE, width)):
            applied = dot(root[last, 0, start:stop, :], blocks[slot])
            blocks[flipped, start:stop, :] = applied.astype(jnp.bfloat16)
        for start, stop in panels(min(TILE, width)):
            value = dot(blocks[flipped, start:stop, :], root[last, 1])
            product[slot, start:stop, :] = value.astype(jnp.bfloat16)
            sums[0] += fold(value * value)

        @pl.when(slot == slots - 1)
        def _():
            for k in range(owners):
                piece(k).start()

    both = jnp.concatenate([lane_fold(sums[0]), lane_fold(sums[1])], axis=0)
    send_sums(1, over_mp, mp_ratio, both)
    send_sums(1, over_dp, dp_ratio, total_sums(1, over_mp, mp_ratio))
    totals = total_sums(1, over_dp, dp_ratio)
    ratio = jnp.sqrt(whole_sum(totals[8:]) / (whole_sum(totals[:8]) + 1e-06))
    ratio_ref[...] = jnp.broadcast_to(ratio, ratio_ref.shape)
    for k in near_first:
        for slot in range(slots):
            rows_in(slot, k).wait_send()
        rows_out(k).wait()
    own_out.wait()
    for k in range(owners):
        piece(k).wait()


def refresh(gradients, statistics, accumulator, owners, shards, entries):
    slots = statistics.shape[0] // 2
    dev_rows, width = gradients.shape[-2:]
    hbm = pl.BlockSpec(memory_space=pl.ANY)
    vmem = pl.BlockSpec(memory_space=pltpu.VMEM)
    tile = jax.ShapeDtypeStruct((8, 128), jnp.float32)
    dma = pltpu.SemaphoreType.DMA
    bf16 = lambda *lead: pltpu.VMEM((*lead, width, width), jnp.bfloat16)
    f32 = lambda *shape: pltpu.VMEM(shape, jnp.float32)
    return pl.pallas_call(
        lambda *refs: refresh_kernel(owners, shards, dev_rows, entries, *refs),
        out_shape=(
            jax.ShapeDtypeStruct(statistics.shape, jnp.float32),
            jax.ShapeDtypeStruct((width, width), jnp.bfloat16),
            *[jax.ShapeDtypeStruct((dev_rows, width), jnp.bfloat16)] * owners,
            tile,
            tile,
        ),
        in_specs=[hbm] * 3,
        out_specs=(hbm, hbm, *[hbm] * owners, vmem, vmem),
        scratch_shapes=[
            f32(2, width, width),
            bf16(slots + 1),
            pltpu.VMEM((2 * width, width), jnp.bfloat16),
            bf16(2),
            bf16(2),
            bf16(2, 2),
            bf16(2, 2),
            bf16(slots),
            f32(slots * width, width),
            f32(2, 8, width),
            f32(2, 8, width),
            f32(owners, 8, 128),
            f32(shards, 8, 128),
            f32(owners, 16, 128),
            f32(shards, 16, 128),
            dma((slots, owners)),
            dma((slots, owners)),
            dma((owners,)),
            dma((owners,)),
            dma((2, owners)),
            dma((2, owners)),
            dma((2, shards)),
            dma((2, shards)),
            dma((2,)),
            dma((slots + 1,)),
            dma((2,)),
            dma((2,)),
            dma((owners,)),
            pltpu.SemaphoreType.REGULAR,
        ],
        compiler_params=pltpu.CompilerParams(
            collective_id=0, has_side_effects=True, vmem_limit_bytes=63 * 2**20
        ),
        cost_estimate=pl.CostEstimate(
            flops=60 * width**3, bytes_accessed=40 * width**2, transcendentals=0
        ),
        name="refresh",
    )(
        gradients.reshape(slots * width, width),
        statistics,
        accumulator.reshape(slots * width, width),
    )


def settle_kernel(ratio_ref, clip_ref, stats_ref, grad_ref, accum_ref, back_ref, *outs):
    stats_out, accum_out, update_out = outs
    stats_out[...] = stats_ref[...]
    scaled = clip_ref[0:1, 0:1] * grad_ref[...].astype(jnp.float32)
    accum_out[...] = accum_ref[...] + scaled * scaled
    update_out[0, 0] = ratio_ref[0:1, 0:1] * back_ref[...].astype(jnp.float32)


def settle(ratio, clip, stats, grads, accum, returned, owners, slots):
    factors, width, _ = stats.shape
    dev_rows = width // owners
    steps = 2 * owners
    stat_rows = factors * width // steps
    per_stat = width // stat_rows
    half = dev_rows // 2
    rows = lambda count: pl.BlockSpec((count, width), lambda i: (i, 0))
    tile = pl.BlockSpec((8, 128), lambda i: (0, 0))
    stat = pl.BlockSpec((1, stat_rows, width), lambda i: (i // per_stat, i % per_stat, 0))
    grad_rows = grads.shape[0] // steps
    return pl.pallas_call(
        settle_kernel,
        grid=(steps,),
        out_shape=(
            jax.ShapeDtypeStruct(stats.shape, jnp.float32),
            jax.ShapeDtypeStruct(accum.shape, jnp.float32),
            jax.ShapeDtypeStruct((owners, slots, dev_rows, width), jnp.float32),
        ),
        in_specs=[tile, tile, stat, rows(grad_rows), rows(grad_rows), rows(half)],
        out_specs=(
            stat,
            rows(grad_rows),
            pl.BlockSpec((1, 1, half, width), lambda i: (i // 2, 0, i % 2, 0)),
        ),
        cost_estimate=pl.CostEstimate(
            flops=40 * width**3 // 4, bytes_accessed=58 * width**2, transcendentals=0
        ),
        name="settle",
    )(ratio, clip, stats, grads, accum, returned)


def power_of_two(count):
    return count >= 2 and count & (count - 1) == 0


def on_device(gradients, statistics, accumulator):
    owned_factors = statistics.shape[1]
    owners, shards = lax.axis_size("dp"), lax.axis_size("mp")
    row_blocks, col_blocks, dev_rows, block_width = gradients.shape
    paired = owned_factors == 4 and power_of_two(owners) and power_of_two(shards)
    if not paired or dev_rows % CHUNK or block_width % TILE:
        return split_device(gradients, statistics, accumulator)
    slots = owned_factors // 2
    blocks = row_blocks * col_blocks
    entries = float(blocks * dev_rows * block_width * owners * shards)
    results = refresh(gradients, statistics[0], accumulator, owners, shards, entries)
    statistics_new, returned = results[:2]
    pieces = results[2 : 2 + owners]
    ratio, clip = results[2 + owners :]
    arrived = {0: pieces[0]}
    for k in range(1, owners):
        pairs = [(i, i ^ k) for i in range(owners)]
        arrived[k] = lax.ppermute(pieces[k], "dp", pairs)
    flat = lambda value: value.reshape(slots * block_width, block_width)
    statistics_new, accumulated, update = settle(
        ratio, clip, statistics_new, flat(gradients), flat(accumulator), returned, owners, slots
    )
    me = lax.axis_index("dp")
    for k in range(owners):
        rows = ratio[:1, :1] * arrived[k].astype(jnp.float32)
        place = (me ^ k, slots - 1, 0, 0)
        update = lax.dynamic_update_slice(update, rows[None, None], place)
    update = update.reshape(gradients.shape)
    return (update, statistics_new[None], accumulated.reshape(accumulator.shape))


def solution(mesh):
    return jax.shard_map(
        on_device,
        mesh=mesh,
        in_specs=(P(None, "mp", "dp", None), P("mp", "dp", None, None), P(None, "mp", "dp", None)),
        out_specs=(P(None, "mp", "dp", None), P("mp", "dp", None, None), P(None, "mp", "dp", None)),
        check_vma=False,
    )
```

```python
import jax
import jax.numpy as jnp
from jax import lax
from jax.experimental import pallas as pl
from jax.experimental.pallas import tpu as pltpu
from jax.sharding import PartitionSpec as P

ITERS = 3


def partner_2(value, axis, distance):
    return lax.ppermute(value, axis, [(i, i ^ 1 << distance) for i in range(lax.axis_size(axis))])


def batch_dot(left, right):
    return jnp.einsum("kij,kjl->kil", left, right, preferred_element_type=jnp.float32)


def inverse_roots(statistic):
    block_width = statistic.shape[-1]
    identity = jnp.eye(block_width, dtype=jnp.float32)
    frob_norms = jnp.sqrt(jnp.sum(statistic * statistic, axis=(1, 2)) + 1e-06)
    newton_scale = (2.5 / frob_norms)[:, None, None]
    matrix = newton_scale * statistic
    root_iter = jnp.sqrt(jnp.sqrt(newton_scale)) * identity
    for iteration in range(ITERS):
        factor = (1.25 * identity - 0.25 * matrix).astype(jnp.bfloat16)
        root_iter = batch_dot(root_iter.astype(jnp.bfloat16), factor)
        if iteration + 1 < ITERS:
            square = batch_dot(factor, factor).astype(jnp.bfloat16)
            fourth = batch_dot(square, square).astype(jnp.bfloat16)
            matrix = batch_dot(fourth, matrix.astype(jnp.bfloat16))
    return root_iter


def split_device(gradients, statistics, accumulator):
    owners = lax.axis_size("dp")
    own_index = lax.axis_index("dp")
    row_blocks, col_blocks, dev_rows, block_width = gradients.shape
    blocks = row_blocks * col_blocks
    owned_factors = statistics.shape[1]
    split_pairs = owned_factors == 1
    half_rows = dev_rows // 2
    parity = own_index % 2
    left_side = parity == 0
    by_block = gradients.reshape(blocks, dev_rows, block_width)
    grads_wide = gradients.astype(jnp.float32)
    grad_total = lax.psum(jnp.sum(grads_wide * grads_wide), ("dp", "mp"))
    entries = blocks * dev_rows * block_width * owners * lax.axis_size("mp")
    clip_factor = jnp.minimum(1.0, jnp.sqrt(entries / (grad_total + 1e-06)))
    scaled = clip_factor * grads_wide
    accumulated = accumulator + scaled * scaled
    graft_step = scaled / jnp.sqrt(accumulated)
    graft_squares = jnp.sum(graft_step * graft_step)
    row_parts = 2 if split_pairs else 1
    row_units = by_block.reshape(blocks * row_parts, dev_rows // row_parts, block_width)
    received = lax.all_to_all(row_units, "dp", split_axis=0, concat_axis=1, tiled=True)
    if split_pairs:
        partner_part = partner_2(received, "dp", 0)
        own_part = received.reshape(owners, 1, half_rows, block_width)
        partner_part = partner_part.reshape(owners, 1, half_rows, block_width)
        ordered = jnp.where(
            left_side,
            jnp.concatenate([own_part, partner_part], 1),
            jnp.concatenate([partner_part, own_part], 1),
        )
        whole_blocks = ordered.reshape(1, owners * dev_rows, block_width)
    else:
        whole_blocks = received
    transposed = jnp.swapaxes(whole_blocks, 1, 2)
    if split_pairs:
        factor_inputs = jnp.where(left_side, whole_blocks, transposed)
    else:
        factor_inputs = jnp.stack([whole_blocks, transposed], 1).reshape(
            owned_factors, block_width, block_width
        )
    gram_matrix = jnp.einsum(
        "kij,klj->kil", factor_inputs, factor_inputs, preferred_element_type=jnp.float32
    )
    statistics_new = (
        0.9 * statistics[0] + 0.1 / block_width * clip_factor * clip_factor * gram_matrix
    )
    root_values = inverse_roots(statistics_new).astype(jnp.bfloat16)
    if split_pairs:
        partner = partner_2(root_values, "dp", 0)
        left_root = jnp.where(left_side, root_values, partner)[0]
        right_root = jnp.where(left_side, partner, root_values)[0]
        left_rows = lax.dynamic_slice_in_dim(
            left_root.reshape(owners, 2, half_rows, block_width), parity, 1, 1
        )
        left_rows = left_rows.reshape(owners * half_rows, block_width)
        left_applied = jnp.dot(
            left_rows, whole_blocks[0], preferred_element_type=jnp.float32
        ).astype(jnp.bfloat16)
        product = jnp.dot(left_applied, right_root, preferred_element_type=jnp.float32)
        pieces = product.reshape(1, owners, half_rows, block_width)
    else:
        root_pairs = root_values.reshape(-1, 2, block_width, block_width)
        left_applied = batch_dot(root_pairs[:, 0], whole_blocks).astype(jnp.bfloat16)
        product = batch_dot(left_applied, root_pairs[:, 1])
        pieces = product.reshape(-1, owners, dev_rows, block_width)
    returned = lax.all_to_all(
        pieces.astype(jnp.bfloat16), "dp", split_axis=1, concat_axis=0, tiled=True
    ).astype(pieces.dtype)
    returned = returned.reshape(row_blocks, col_blocks, dev_rows, block_width)
    graft_total, update_total = lax.psum(
        (graft_squares, jnp.sum(returned * returned)), ("dp", "mp")
    )
    graft_ratio = jnp.sqrt(graft_total / (update_total + 1e-06))
    return (graft_ratio * returned, statistics_new[None], accumulated)


TILE = 512
FINE_TILE = 256
CHUNK = 128
MESH = pl.DeviceIdType.MESH


def peer_of(index, distance):
    bit, other = 1, index
    while bit <= distance:
        if distance & bit:
            other = other + bit * (1 - 2 * ((index // bit) % 2))
        bit *= 2
    return other


def fold(squares):
    rows, width = squares.shape
    return jnp.sum(squares.reshape(rows // 8, 8, width), axis=0)


def lane_fold(sums):
    total = sums[:, :128]
    for start in range(128, sums.shape[1], 128):
        total = total + sums[:, start : start + 128]
    return total


def whole_sum(tile):
    return jnp.sum(jnp.sum(tile, axis=0, keepdims=True), axis=1, keepdims=True)


def refresh_kernel(owners, shards, dev_rows, entries, *refs):
    grad_hbm, stats_hbm, accum_hbm = refs[:3]
    out_stats, returned = refs[3:5]
    pieces = refs[5 : 5 + owners]
    ratio_ref, clip_ref = refs[5 + owners : 7 + owners]
    (stat, blocks, factor, square, fourth, mats, root, product, accum, frob, sums) = refs[
        7 + owners : 18 + owners
    ]
    (dp_clip, mp_clip, dp_ratio, mp_ratio) = refs[18 + owners : 22 + owners]
    (
        in_send, in_recv, out_send, out_recv, dp_send, dp_recv, mp_send, mp_recv,
        stage_sem, own_sem, load_sem, store_sem, piece_sem, turn_sem,
    ) = refs[22 + owners :]
    width = grad_hbm.shape[1]
    slots = grad_hbm.shape[0] // width
    me, shard = lax.axis_index("dp"), lax.axis_index("mp")
    dot = lambda a, b: jnp.dot(a, b, preferred_element_type=jnp.float32)
    near_first = list(range(1, owners))
    partner = peer_of(me, max(1, owners // 4))
    flipped = slots

    def start_all(copy_of):
        for k in near_first:
            copy_of(k).start()

    def rows_of(owner):
        return pl.ds(pl.multiple_of(owner * dev_rows, dev_rows), dev_rows)

    def unit(owner, slot):
        start = (owner * slots + slot) * dev_rows
        return grad_hbm.at[pl.ds(pl.multiple_of(start, dev_rows), dev_rows)]

    def own_rows(slot):
        return pltpu.make_async_copy(
            unit(me, slot), blocks.at[slot, rows_of(me)], own_sem.at[slot]
        )

    def rows_in(slot, k):
        return pltpu.make_async_remote_copy(
            src_ref=unit(peer_of(me, k), slot),
            dst_ref=blocks.at[slot, rows_of(me)],
            send_sem=in_send.at[slot, k],
            recv_sem=in_recv.at[slot, k],
            device_id=(peer_of(me, k), shard),
            device_id_type=MESH,
        )

    def rows_out(k):
        return pltpu.make_async_remote_copy(
            src_ref=product.at[0, rows_of(peer_of(me, k))],
            dst_ref=returned.at[rows_of(me)],
            send_sem=out_send.at[k],
            recv_sem=out_recv.at[k],
            device_id=(peer_of(me, k), shard),
            device_id_type=MESH,
        )

    def piece(k):
        source = product.at[slots - 1, rows_of(peer_of(me, k))]
        return pltpu.make_async_copy(source, pieces[k], piece_sem.at[k])

    own_out = pltpu.make_async_copy(
        product.at[0, rows_of(me)], returned.at[rows_of(me)], own_sem.at[slots]
    )

    def load(slot, s):
        return pltpu.make_async_copy(
            stats_hbm.at[2 * slot + s], stat.at[s], load_sem.at[s]
        )

    def store(slot, s):
        return pltpu.make_async_copy(
            stat.at[s], out_stats.at[2 * slot + s], store_sem.at[s]
        )

    def dp_copy(which, buffer, k):
        return pltpu.make_async_remote_copy(
            src_ref=buffer.at[me],
            dst_ref=buffer.at[me],
            send_sem=dp_send.at[which, k],
            recv_sem=dp_recv.at[which, k],
            device_id=(peer_of(me, k), shard),
            device_id_type=MESH,
        )

    def mp_copy(which, buffer, k):
        return pltpu.make_async_remote_copy(
            src_ref=buffer.at[shard],
            dst_ref=buffer.at[shard],
            send_sem=mp_send.at[which, k],
            recv_sem=mp_recv.at[which, k],
            device_id=(me, peer_of(shard, k)),
            device_id_type=MESH,
        )

    over_dp = (dp_copy, me, near_first)
    over_mp = (mp_copy, shard, list(range(1, shards)))

    def send_sums(which, axis, buffer, tile):
        copy_of, place, distances = axis
        buffer[place] = tile
        for k in distances:
            copy_of(which, buffer, k).start()

    def total_sums(which, axis, buffer):
        copy_of, _, distances = axis
        for k in distances:
            copy_of(which, buffer, k).wait()
        return jnp.sum(buffer[...], axis=0)

    stage_grads = pltpu.make_async_copy(grad_hbm, factor, stage_sem.at[0])
    stage_accum = pltpu.make_async_copy(accum_hbm, accum, stage_sem.at[1])
    stage_grads.start()
    barrier = pltpu.get_barrier_semaphore()
    for k in range(1, owners):
        pl.semaphore_signal(
            barrier, inc=1, device_id=(peer_of(me, k), shard), device_id_type=MESH
        )
    for k in range(1, shards):
        pl.semaphore_signal(
            barrier, inc=1, device_id=(me, peer_of(shard, k)), device_id_type=MESH
        )
    pl.semaphore_wait(barrier, owners + shards - 2)

    stage_grads.wait()
    sums[0] = jnp.zeros((8, width), jnp.float32)

    @pl.loop(0, slots * width // CHUNK)
    def _(i):
        rows = pl.ds(pl.multiple_of(i * CHUNK, CHUNK), CHUNK)
        wide = factor[rows, :].astype(jnp.float32)
        sums[0] += fold(wide * wide)

    send_sums(0, over_dp, dp_clip, lane_fold(sums[0]))
    start_all(lambda k: rows_in(0, k))
    for slot in range(slots):
        own_rows(slot).start()
    stage_accum.start()
    for s in range(2):
        load(0, s).start()

    send_sums(0, over_mp, mp_clip, total_sums(0, over_dp, dp_clip))
    grad_total = whole_sum(total_sums(0, over_mp, mp_clip))
    clip_factor = jnp.minimum(1.0, jnp.sqrt(entries / (grad_total + 1e-06)))
    clip_ref[...] = clip_factor
    sums[0] = jnp.zeros((8, width), jnp.float32)
    sums[1] = jnp.zeros((8, width), jnp.float32)
    stage_accum.wait()

    @pl.loop(0, slots * width // CHUNK)
    def _(i):
        rows = pl.ds(pl.multiple_of(i * CHUNK, CHUNK), CHUNK)
        scaled = clip_ref[...] * factor[rows, :].astype(jnp.float32)
        graft_step = scaled / jnp.sqrt(accum[rows, :] + scaled * scaled)
        sums[1] += fold(graft_step * graft_step)

    def panels(tile):
        return [(start, start + tile) for start in range(0, width, tile)]

    def diagonal(rows, cols):
        row_ids = lax.broadcasted_iota(jnp.int32, (rows, cols), 0)
        return row_ids == lax.broadcasted_iota(jnp.int32, (rows, cols), 1)

    def mirrored(write, left, right, tile=FINE_TILE):
        for start, stop in panels(min(tile, width)):
            upper = dot(left[start:stop, :], right[:, start:])
            write(start, stop, upper)

    def keep(target, start, stop, value):
        target[start:stop, start:] = value
        if stop < width:
            target[stop:, start:stop] = value[:, stop - start :].T

    @pl.loop(0, slots)
    def _(slot):
        own_rows(slot).wait()
        for k in range(owners):
            if k:
                rows_in(slot, k).wait_recv()
            rows = rows_of(peer_of(me, k))
            blocks[flipped, :, rows] = blocks[slot, rows, :].T

        @pl.when(slot + 1 < slots)
        def _():
            pl.semaphore_signal(
                turn_sem, inc=1, device_id=(partner, shard), device_id_type=MESH
            )
            pl.semaphore_wait(turn_sem, 1)
            start_all(lambda k: rows_in(slot + 1, k))

        @pl.when(slot == 1)
        def _():
            pl.semaphore_signal(
                turn_sem, inc=1, device_id=(partner, shard), device_id_type=MESH
            )
            pl.semaphore_wait(turn_sem, 1)
            start_all(rows_out)
            own_out.start()

        for s in range(2):
            load(slot, s).wait()

        @pl.loop(0, 2)
        def _(s):
            left = blocks.at[slot + s * (flipped - slot)]
            right = blocks.at[flipped - s * (flipped - slot)]
            old = stat.at[s]
            clip = clip_ref[...]
            scale = 0.1 / width * clip * clip
            frob[s] = jnp.zeros((8, width), jnp.float32)

            def write(start, stop, upper):
                part = scale * upper
                new = 0.9 * old[start:stop, start:] + part
                old[start:stop, start:] = new
                frob[s, :, start:] += fold(new * new)
                if stop < width:
                    new = 0.9 * old[stop:, start:stop] + part[:, stop - start :].T
                    old[stop:, start:stop] = new
                    frob[s, :, start:stop] += fold(new * new)

            mirrored(write, left, right)
            store(slot, s).start()

        @pl.loop(0, 2)
        def _(s):
            newton_scale = 2.5 / jnp.sqrt(whole_sum(frob[s]) + 1e-06)
            first_root = jnp.sqrt(jnp.sqrt(newton_scale))
            first_root = first_root.astype(jnp.bfloat16).astype(jnp.float32)

            @pl.loop(0, width // CHUNK)
            def _(i):
                row = pl.multiple_of(i * CHUNK, CHUNK)
                rows = pl.ds(row, CHUNK)
                wide = pl.ds(pl.multiple_of(s * width + row, CHUNK), CHUNK)
                matrix = newton_scale * stat[s, rows, :]
                value = (-0.25 * matrix).astype(jnp.bfloat16)
                factor[wide, :] = value
                root[0, s, rows, :] = (first_root * value.astype(jnp.float32)).astype(
                    jnp.bfloat16
                )
                mats[0, s, rows, :] = matrix.astype(jnp.bfloat16)
                quarter = -0.25 * (newton_scale * stat[s, rows, rows])
                value = jnp.where(diagonal(CHUNK, CHUNK), 1.25 + quarter, quarter)
                value = value.astype(jnp.bfloat16)
                factor[wide, rows] = value
                root[0, s, rows, rows] = (first_root * value.astype(jnp.float32)).astype(
                    jnp.bfloat16
                )

        @pl.loop(0, ITERS - 1)
        def _(step):
            now = lax.rem(step, 2)
            later = 1 - now

            def each(body):
                for s in range(2):
                    body(s, factor.at[s * width : (s + 1) * width])

            def squared(s, own):
                def write(start, stop, upper):
                    keep(square.at[s], start, stop, upper.astype(jnp.bfloat16))

                mirrored(write, own, own)

            def power(s, own):
                def write(start, stop, upper):
                    keep(fourth.at[s], start, stop, upper.astype(jnp.bfloat16))

                mirrored(write, square.at[s], square.at[s])

            def next_matrix(s, own):
                def write(start, stop, upper):
                    quarter = -0.25 * upper
                    on_diagonal = diagonal(*upper.shape)
                    value = jnp.where(on_diagonal, 1.25 + quarter, quarter)
                    keep(own, start, stop, value.astype(jnp.bfloat16))
                    keep(mats.at[later, s], start, stop, upper.astype(jnp.bfloat16))

                mirrored(write, fourth.at[s], mats.at[now, s], TILE)

            def next_root(s, own):
                def write(start, stop, upper):
                    keep(root.at[later, s], start, stop, upper.astype(jnp.bfloat16))

                mirrored(write, root.at[now, s], own, TILE)

            each(squared)
            each(power)
            each(next_matrix)
            each(next_root)

        for s in range(2):
            store(slot, s).wait()

        @pl.when(slot + 1 < slots)
        def _():
            for s in range(2):
                load(slot + 1, s).start()

        last = (ITERS - 1) % 2
        for start, stop in panels(min(TILE, width)):
            applied = dot(root[last, 0, start:stop, :], blocks[slot])
            blocks[flipped, start:stop, :] = applied.astype(jnp.bfloat16)
        for start, stop in panels(min(TILE, width)):
            value = dot(blocks[flipped, start:stop, :], root[last, 1])
            product[slot, start:stop, :] = value.astype(jnp.bfloat16)
            sums[0] += fold(value * value)

        @pl.when(slot == slots - 1)
        def _():
            for k in range(owners):
                piece(k).start()

    both = jnp.concatenate([lane_fold(sums[0]), lane_fold(sums[1])], axis=0)
    send_sums(1, over_mp, mp_ratio, both)
    send_sums(1, over_dp, dp_ratio, total_sums(1, over_mp, mp_ratio))
    totals = total_sums(1, over_dp, dp_ratio)
    ratio = jnp.sqrt(whole_sum(totals[8:]) / (whole_sum(totals[:8]) + 1e-06))
    ratio_ref[...] = ratio
    for k in near_first:
        for slot in range(slots):
            rows_in(slot, k).wait_send()
        rows_out(k).wait()
    own_out.wait()
    for k in range(owners):
        piece(k).wait()


def refresh(gradients, statistics, accumulator, owners, shards, entries):
    slots = statistics.shape[0] // 2
    dev_rows, width = gradients.shape[-2:]
    hbm = pl.BlockSpec(memory_space=pl.ANY)
    vmem = pl.BlockSpec(memory_space=pltpu.VMEM)
    tile = jax.ShapeDtypeStruct((1, 1), jnp.float32)
    dma = pltpu.SemaphoreType.DMA
    bf16 = lambda *lead: pltpu.VMEM((*lead, width, width), jnp.bfloat16)
    f32 = lambda *shape: pltpu.VMEM(shape, jnp.float32)
    return pl.pallas_call(
        lambda *refs: refresh_kernel(owners, shards, dev_rows, entries, *refs),
        out_shape=(
            jax.ShapeDtypeStruct(statistics.shape, jnp.float32),
            jax.ShapeDtypeStruct((width, width), jnp.bfloat16),
            *[jax.ShapeDtypeStruct((dev_rows, width), jnp.bfloat16)] * owners,
            tile,
            tile,
        ),
        in_specs=[hbm] * 3,
        out_specs=(hbm, hbm, *[hbm] * owners, vmem, vmem),
        scratch_shapes=[
            f32(2, width, width),
            bf16(slots + 1),
            pltpu.VMEM((2 * width, width), jnp.bfloat16),
            bf16(2),
            bf16(2),
            bf16(2, 2),
            bf16(2, 2),
            bf16(slots),
            f32(slots * width, width),
            f32(2, 8, width),
            f32(2, 8, width),
            f32(owners, 8, 128),
            f32(shards, 8, 128),
            f32(owners, 16, 128),
            f32(shards, 16, 128),
            dma((slots, owners)),
            dma((slots, owners)),
            dma((owners,)),
            dma((owners,)),
            dma((2, owners)),
            dma((2, owners)),
            dma((2, shards)),
            dma((2, shards)),
            dma((2,)),
            dma((slots + 1,)),
            dma((2,)),
            dma((2,)),
            dma((owners,)),
            pltpu.SemaphoreType.REGULAR,
        ],
        compiler_params=pltpu.CompilerParams(
            collective_id=0, has_side_effects=True, vmem_limit_bytes=63 * 2**20
        ),
        cost_estimate=pl.CostEstimate(
            flops=60 * width**3, bytes_accessed=40 * width**2, transcendentals=0
        ),
        name="refresh",
    )(
        gradients.reshape(slots * width, width),
        statistics,
        accumulator.reshape(slots * width, width),
    )


def settle_kernel(ratio_ref, clip_ref, stats_ref, grad_ref, accum_ref, back_ref, *outs):
    stats_out, accum_out, update_out = outs
    stats_out[...] = stats_ref[...]
    scaled = clip_ref[...] * grad_ref[...].astype(jnp.float32)
    accum_out[...] = accum_ref[...] + scaled * scaled
    update_out[0, 0] = ratio_ref[...] * back_ref[...].astype(jnp.float32)


def settle(ratio, clip, stats, grads, accum, returned, owners, slots):
    factors, width, _ = stats.shape
    dev_rows = width // owners
    steps = owners
    stat_rows = factors * width // steps
    per_stat = width // stat_rows
    rows = lambda count: pl.BlockSpec((count, width), lambda i: (i, 0))
    tile = pl.BlockSpec((1, 1), lambda i: (0, 0))
    stat = pl.BlockSpec((1, stat_rows, width), lambda i: (i // per_stat, i % per_stat, 0))
    grad_rows = grads.shape[0] // steps
    return pl.pallas_call(
        settle_kernel,
        grid=(steps,),
        out_shape=(
            jax.ShapeDtypeStruct(stats.shape, jnp.float32),
            jax.ShapeDtypeStruct(accum.shape, jnp.float32),
            jax.ShapeDtypeStruct((owners, slots, dev_rows, width), jnp.float32),
        ),
        in_specs=[tile, tile, stat, rows(grad_rows), rows(grad_rows), rows(dev_rows)],
        out_specs=(
            stat,
            rows(grad_rows),
            pl.BlockSpec((1, 1, dev_rows, width), lambda i: (i, 0, 0, 0)),
        ),
        cost_estimate=pl.CostEstimate(
            flops=40 * width**3 // 4, bytes_accessed=58 * width**2, transcendentals=0
        ),
        name="settle",
    )(ratio, clip, stats, grads, accum, returned)


def power_of_two(count):
    return count >= 2 and count & (count - 1) == 0


def on_device(gradients, statistics, accumulator):
    owned_factors = statistics.shape[1]
    owners, shards = lax.axis_size("dp"), lax.axis_size("mp")
    row_blocks, col_blocks, dev_rows, block_width = gradients.shape
    paired = owned_factors == 4 and power_of_two(owners) and power_of_two(shards)
    if not paired or dev_rows % CHUNK or block_width % TILE:
        return split_device(gradients, statistics, accumulator)
    slots = owned_factors // 2
    blocks = row_blocks * col_blocks
    entries = float(blocks * dev_rows * block_width * owners * shards)
    results = refresh(gradients, statistics[0], accumulator, owners, shards, entries)
    statistics_new, returned = results[:2]
    pieces = results[2 : 2 + owners]
    ratio, clip = results[2 + owners :]
    arrived = {0: pieces[0]}
    for k in range(owners - 1, 0, -1):
        pairs = [(i, i ^ k) for i in range(owners)]
        arrived[k] = lax.ppermute(pieces[k], "dp", pairs)
    flat = lambda value: value.reshape(slots * block_width, block_width)
    statistics_new, accumulated, update = settle(
        ratio, clip, statistics_new, flat(gradients), flat(accumulator), returned, owners, slots
    )
    me = lax.axis_index("dp")
    for k in range(owners):
        rows = ratio[0, 0] * arrived[k].astype(jnp.float32)
        place = (me ^ k, slots - 1, 0, 0)
        update = lax.dynamic_update_slice(update, rows[None, None], place)
    update = update.reshape(gradients.shape)
    return (update, statistics_new[None], accumulated.reshape(accumulator.shape))


def solution(mesh):
    return jax.shard_map(
        on_device,
        mesh=mesh,
        in_specs=(P(None, "mp", "dp", None), P("mp", "dp", None, None), P(None, "mp", "dp", None)),
        out_specs=(P(None, "mp", "dp", None), P("mp", "dp", None, None), P(None, "mp", "dp", None)),
        check_vma=False,
    )
```
